32 devices in a mesh: wave: 4 (over y, x), freq: 8 (over z, core).
Axes of the slice: x: 2, y: 2, z: 4, core: 2. Of those that a mesh axis runs over, the one named last changes fastest.
Arguments:
- waveforms: float32 [1024, 16384], P('wave', 'freq'), may hold values from -6 to 6
- pivots: int32 [2, 128], replicated, may hold values from 0 to 1023, as said below
- nodes: int32 [1024], replicated, may hold values from 0 to 16383, as said below
Outputs:
- residual: float32 [1024, 16384], P('wave', 'freq')
- basis_rows: float32 [256, 16384], P(None, 'freq')
- fitted: float32 [1024, 16384], P('wave', 'freq')
The draws below stay inside these ranges and needn't reach their ends.
Inputs may be any that keep to these rules, and one draw needn't show every extreme that they name: `pivots`: all 256 pivot indices are different. `nodes`: all node indices are different.
All inputs are finite; a program needn't handle non-finite values.
Results may differ from the reference program's by a relative error of at most 0.0001.
Values sent between devices are 32-bit elements; how exact they have to be, the bound alone decides.
A program may use at most 64 MiB of HBM per device.

```python
import jax
import jax.numpy as jnp
from jax import lax

F = 16384
B = 128
STEPS = 2
NODES = 1024
M = 1024


def draw_pivots(key, part):
    order = jax.random.permutation(key, M)
    return order[:STEPS * B].reshape(STEPS, B).astype(jnp.int32)


def draw_nodes(key, part):
    order = jax.random.permutation(key, F)
    return order[:NODES].astype(jnp.int32)


def level_of(rng, extent, split, low, high):
    def one(dim, blocks):
        draws = jax.random.uniform(jax.random.fold_in(jax.random.fold_in(rng, 6), dim), (blocks,), jnp.float32, low / len(split), high / len(split))
        return jnp.repeat(jnp.exp(draws), extent[dim] // blocks).reshape((-1,) + (1,) * (len(extent) - dim - 1))

    gain = one(*split[0])
    for cut in split[1:]:
        gain = gain * one(*cut)
    return gain


def noise(key, shape, width, reach, pieces=(), held_as=jnp.bfloat16):
    drawn = jax.random.normal(key, shape, jnp.float32) * width
    if len(pieces) > 0:
        drawn = level_of(key, shape, pieces, -0.22, 0.18) * drawn
    return jnp.clip(drawn, min=-reach, max=reach).astype(held_as)


def setup_inputs(seed: int = 0) -> dict:
    seeds = jax.random.split(jax.random.key(seed), 4)
    waveforms = noise(seeds[0], (M, F), 1.0, 6.0, ((0, 4), (1, 8)), jnp.float32)
    pivots = draw_pivots(jax.random.fold_in(seeds[3], 71), 0)
    nodes = draw_nodes(jax.random.fold_in(seeds[3], 71), 0)
    return {"waveforms": waveforms, "pivots": pivots, "nodes": nodes}


HIGH = lax.Precision.HIGHEST

def reference(waveforms, pivots, nodes):
    residual = waveforms
    blocks = []
    for step in range(STEPS):
        pivot_block = jnp.take(residual, pivots[step], axis=0)
        gram = jnp.dot(pivot_block, pivot_block.T, precision=HIGH)
        factor = jnp.linalg.cholesky(gram)
        ortho = jax.scipy.linalg.solve_triangular(factor, pivot_block, lower=True)
        coeffs = jnp.dot(residual, ortho.T, precision=HIGH)
        residual = residual - jnp.dot(coeffs, ortho, precision=HIGH)
        blocks.append(ortho)
    basis_rows = jnp.concatenate(blocks, axis=0)
    sampled = jnp.take(basis_rows, nodes, axis=1)
    node_gram = jnp.dot(sampled, sampled.T, precision=HIGH)
    cross = jnp.dot(jnp.take(waveforms, nodes, axis=1), sampled.T, precision=HIGH)
    node_factor = jnp.linalg.cholesky(node_gram)
    coefficients = jax.scipy.linalg.cho_solve((node_factor, True), cross.T).T
    fitted = jnp.dot(coefficients, basis_rows, precision=HIGH)
    return (residual, basis_rows, fitted)
```

```python
import jax
import jax.numpy as jnp
from jax import lax
from jax.sharding import PartitionSpec as P

HIGH = lax.Precision.HIGH


def body(waveforms, pivots, nodes):
    rows_here, cols_here = waveforms.shape
    row_start = lax.axis_index("wave") * rows_here
    col_start = lax.axis_index("freq") * cols_here
    picks = pivots.reshape(-1)
    count = picks.shape[0]
    local_rows = picks - row_start
    inside = ((local_rows >= 0) & (local_rows < rows_here)).astype(jnp.float32)
    picked = jnp.take(waveforms, jnp.clip(local_rows, 0, rows_here - 1), axis=0) * inside[:, None]
    pivot_rows = lax.psum(picked, "wave")
    columns = col_start + jnp.arange(cols_here, dtype=jnp.int32)
    node_count = jnp.sum((nodes[:, None] == columns[None, :]).astype(jnp.float32), axis=0)
    weighted = pivot_rows * node_count[None, :]
    left = jnp.concatenate([pivot_rows, waveforms], axis=0)
    right = jnp.concatenate([pivot_rows, weighted], axis=0)
    total = lax.psum(jnp.dot(left, right.T, precision=HIGH), "freq")
    gram, node_gram = total[:count, :count], total[:count, count:]
    cross, node_cross = total[count:, :count], total[count:, count:]
    factors = jnp.linalg.cholesky(jnp.stack([gram, node_gram]))
    eye = jnp.broadcast_to(jnp.eye(count, dtype=jnp.float32), factors.shape)
    inverses = jax.scipy.linalg.solve_triangular(factors, eye, lower=True)
    hi = lax.Precision.HIGHEST
    basis_rows = jnp.dot(inverses[0], pivot_rows, precision=HIGH)
    coeffs = jnp.dot(cross, inverses[0].T, precision=hi)
    residual = waveforms - jnp.dot(coeffs, basis_rows, precision=HIGH)
    coefficients = jnp.dot(jnp.dot(node_cross, inverses[1].T, precision=hi), inverses[1], precision=hi)
    fitted = jnp.dot(coefficients, pivot_rows, precision=HIGH)
    return (residual, basis_rows, fitted)


def solution(mesh):
    in_specs = (P("wave", "freq"), P(), P())
    out_specs = (P("wave", "freq"), P(None, "freq"), P("wave", "freq"))
    return jax.shard_map(body, mesh=mesh, in_specs=in_specs, out_specs=out_specs, check_vma=False)
```

```python
import functools

import jax
import jax.numpy as jnp
from jax import lax
from jax.experimental import pallas as pl
from jax.experimental.pallas import tpu as pltpu
from jax.sharding import PartitionSpec as P

HIGH = lax.Precision.HIGH
FULL = lax.Precision.HIGHEST
MESH = pl.DeviceIdType.MESH
VMEM = pl.BlockSpec(memory_space=pltpu.VMEM)
SMEM = pl.BlockSpec(memory_space=pltpu.SMEM)


def dot(a, b):
    return lax.dot_general(
        a, b, (((1,), (0,)), ((), ())), precision=FULL, preferred_element_type=jnp.float32
    )


def dot_t(a, b):
    return lax.dot_general(
        a, b, (((1,), (1,)), ((), ())), precision=FULL, preferred_element_type=jnp.float32
    )


def factor_kernel(steps, size, total_ref, out_ref, work):
    count = steps * size
    subs = lax.broadcasted_iota(jnp.int32, (size, size), 0)
    lanes = lax.broadcasted_iota(jnp.int32, (size, size), 1)
    lane = lax.broadcasted_iota(jnp.int32, (1, size), 1)

    def block(m, i, j):
        return total_ref[i * size : (i + 1) * size, m * count + j * size : m * count + (j + 1) * size]

    mats = [[[block(m, i, j) for j in range(i + 1)] for i in range(steps)] for m in range(2)]
    lower = [{} for _ in range(2)]
    inverse = [{} for _ in range(2)]

    def eliminate(j, carry):
        for m in range(2):
            now = work[m]
            row = work[m, pl.ds(j, 1), :]
            here = lanes == j
            col = jnp.sum(jnp.where(here, now, 0.0), axis=1, keepdims=True)
            pivot = jnp.sum(jnp.where(lane == j, row, 0.0), axis=1, keepdims=True)
            row = jnp.where(lane == j, 1.0, row) / pivot
            below = subs > j
            work[m] = jnp.where(here & below, 0.0, now) - jnp.where(below, col, 0.0) * row
        return carry

    for b in range(steps):
        for m in range(2):
            work[m] = mats[m][b][b]
        lax.fori_loop(0, size, eliminate, 0)
        for m in range(2):
            done = work[m]
            diag = jnp.sum(jnp.where(subs == lanes, done, 0.0), axis=1, keepdims=True)
            unit = jnp.where(subs > lanes, done, jnp.where(subs == lanes, 1.0, 0.0))
            inverse[m][b, b] = unit / jnp.sqrt(diag)
            for i in range(b + 1, steps):
                lower[m][i, b] = dot_t(mats[m][i][b], inverse[m][b, b])
            for i in range(b + 1, steps):
                for j in range(b + 1, i + 1):
                    mats[m][i][j] = mats[m][i][j] - dot_t(lower[m][i, b], lower[m][j, b])
    for m in range(2):
        for j in range(steps):
            for i in range(j + 1, steps):
                acc = dot(lower[m][i, j], inverse[m][j, j])
                for k in range(j + 1, i):
                    acc = acc + dot(lower[m][i, k], inverse[m][k, j])
                inverse[m][i, j] = -dot(inverse[m][i, i], acc)
    zero = jnp.zeros((size, size), jnp.float32)
    full = [
        jnp.concatenate(
            [jnp.concatenate([inverse[m].get((i, j), zero) for j in range(steps)], axis=1) for i in range(steps)],
            axis=0,
        )
        for m in range(2)
    ]
    out_ref[:count, :] = full[0]
    rows = total_ref.shape[0] - count
    out_ref[count : count + rows, :] = dot(dot_t(total_ref[count:, :count], full[0]), full[0])
    out_ref[count + rows :, :] = dot(dot_t(total_ref[count:, count:], full[1]), full[1])


def factor(total, steps, size):
    count = steps * size
    rows = total.shape[0] - count
    return pl.pallas_call(
        functools.partial(factor_kernel, steps, size),
        out_shape=jax.ShapeDtypeStruct((count + 2 * rows, count), jnp.float32),
        in_specs=[VMEM],
        out_specs=VMEM,
        scratch_shapes=[pltpu.VMEM((2, size, size), jnp.float32)],
    )(total)


def freq_kernel(chips, part_ref, out_ref, half, near, far, send, recv):
    wave, freq = lax.axis_index("wave"), lax.axis_index("freq")
    core, chip = lax.rem(freq, 2), lax.div(freq, 2)
    rows = part_ref.shape[0]
    mid, piece = rows // 2, rows // 2 // chips
    mate = (wave, chip * 2 + 1 - core)
    others = [(wave, lax.rem(chip + d, chips) * 2 + core) for d in range(1, chips)]
    barrier = pltpu.get_barrier_semaphore()
    for peer in [mate] + others:
        pl.semaphore_signal(barrier, inc=1, device_id=peer, device_id_type=MESH)
    pl.semaphore_wait(barrier, chips)

    def copy(slot, src, dst, peer):
        return pltpu.make_async_remote_copy(
            src_ref=src, dst_ref=dst, send_sem=send.at[slot], recv_sem=recv.at[slot],
            device_id=peer, device_id_type=MESH,
        )

    def span(owner_core, owner_chip):
        return pl.ds(pl.multiple_of(owner_core * mid + owner_chip * piece, 8), piece)

    first = copy(0, part_ref.at[pl.ds(pl.multiple_of((1 - core) * mid, 8), mid)], near, mate)
    first.start()
    first.wait()
    half[...] = part_ref[pl.ds(pl.multiple_of(core * mid, 8), mid), :] + near[...]
    scatter = []
    for d in range(1, chips):
        to = lax.rem(chip + d, chips)
        scatter.append(
            copy(d, half.at[pl.ds(pl.multiple_of(to * piece, 8), piece)], far.at[d - 1], others[d - 1])
        )
        scatter[-1].start()
    for c in scatter:
        c.wait()
    total = half[pl.ds(pl.multiple_of(chip * piece, 8), piece), :]
    for d in range(1, chips):
        total = total + far[d - 1]
    out_ref[span(core, chip), :] = total
    own = out_ref.at[span(core, chip)]
    gather = [copy(chips + d - 1, own, own, others[d - 1]) for d in range(1, chips)]
    for c in gather:
        c.start()
    relay = [copy(2 * chips - 1, own, own, mate)]
    relay[0].start()
    for d in range(1, chips):
        gather[d - 1].wait_recv()
        came = out_ref.at[span(core, lax.rem(chip - d + chips, chips))]
        relay.append(copy(2 * chips - 1 + d, came, came, mate))
        relay[-1].start()
    for c in gather:
        c.wait_send()
    for c in relay:
        c.wait()


def freq_sum(part, freq, ident):
    chips = freq // 2
    rows, cols = part.shape
    slots = 3 * chips - 1
    return pl.pallas_call(
        functools.partial(freq_kernel, chips),
        out_shape=jax.ShapeDtypeStruct(part.shape, part.dtype),
        in_specs=[VMEM],
        out_specs=VMEM,
        scratch_shapes=[
            pltpu.VMEM((rows // 2, cols), jnp.float32),
            pltpu.VMEM((rows // 2, cols), jnp.float32),
            pltpu.VMEM((chips - 1, rows // 2 // chips, cols), jnp.float32),
            pltpu.SemaphoreType.DMA((slots,)),
            pltpu.SemaphoreType.DMA((slots,)),
        ],
        compiler_params=pltpu.CompilerParams(collective_id=ident, has_side_effects=True),
    )(part)


def wave_kernel(take_ref, slot_ref, rows_ref, out_ref, packed, gathered, send, recv, here):
    wave, freq = lax.axis_index("wave"), lax.axis_index("freq")
    y, x = lax.div(wave, 2), lax.rem(wave, 2)
    w_x, w_y = y * 2 + 1 - x, (1 - y) * 2 + x
    cap = packed.shape[0]
    mid = cap // 2
    barrier = pltpu.get_barrier_semaphore()
    for w in (w_x, w_y):
        pl.semaphore_signal(barrier, inc=1, device_id=(w, freq), device_id_type=MESH)

    def pack(k, carry):
        packed[pl.ds(k, 1), :] = rows_ref[pl.ds(take_ref[k], 1), :]
        return carry

    lax.fori_loop(0, cap, pack, 0, unroll=8)
    pl.semaphore_wait(barrier, 2)

    def place(owner, part):
        return gathered.at[pl.ds(pl.multiple_of(owner * cap + part * mid, 8), mid)]

    def copy(slot, src, dst, w):
        return pltpu.make_async_remote_copy(
            src_ref=src, dst_ref=dst, send_sem=send.at[slot], recv_sem=recv.at[slot],
            device_id=(w, freq), device_id_type=MESH,
        )

    def own(part):
        return packed.at[pl.ds(part * mid, mid)]

    x0, x1 = copy(0, own(0), place(wave, 0), w_x), copy(1, own(1), place(wave, 1), w_x)
    y1, y0 = copy(2, own(1), place(wave, 1), w_y), copy(3, own(0), place(wave, 0), w_y)
    for c in (x0, y1, x1, y0):
        c.start()
    stay = pltpu.make_async_copy(packed, gathered.at[pl.ds(pl.multiple_of(wave * cap, 8), cap)], here)
    stay.start()
    x0.wait_recv()
    fy = copy(4, place(w_x, 0), place(w_x, 0), w_y)
    fy.start()
    y1.wait_recv()
    fx = copy(5, place(w_y, 1), place(w_y, 1), w_x)
    fx.start()
    x1.wait_recv()
    y0.wait_recv()
    stay.wait()
    fy.wait_recv()
    fx.wait_recv()
    for c in (x0, x1, y0, y1, fx, fy):
        c.wait_send()

    def unpack(k, carry):
        out_ref[pl.ds(k, 1), :] = gathered[pl.ds(slot_ref[k], 1), :]
        return carry

    lax.fori_loop(0, out_ref.shape[0], unpack, 0, unroll=8)


def wave_rows(cap, ident, waves, wave, owner, rank, local_rows, waveforms):
    count = owner.shape[0]
    cols = waveforms.shape[1]
    order = jnp.arange(cap, dtype=jnp.int32)
    mine = (owner == wave)[None, :] & (rank[None, :] == order[:, None])
    take = jnp.sum(jnp.where(mine, local_rows[None, :], 0), axis=1)
    slot = owner * cap + rank
    return pl.pallas_call(
        wave_kernel,
        out_shape=jax.ShapeDtypeStruct((count, cols), jnp.float32),
        in_specs=[SMEM, SMEM, VMEM],
        out_specs=VMEM,
        scratch_shapes=[
            pltpu.VMEM((cap, cols), jnp.float32),
            pltpu.VMEM((waves * cap, cols), jnp.float32),
            pltpu.SemaphoreType.DMA((6,)),
            pltpu.SemaphoreType.DMA((6,)),
            pltpu.SemaphoreType.DMA,
        ],
        compiler_params=pltpu.CompilerParams(collective_id=ident, has_side_effects=True),
    )(take, slot, waveforms)


def gather_pivots(waveforms, picks, waves):
    rows_here = waveforms.shape[0]
    count = picks.shape[0]
    wave = lax.axis_index("wave")
    owner = lax.div(picks, rows_here)
    local_rows = lax.rem(picks, rows_here)
    if waves == 4:
        same = owner[:, None] == owner[None, :]
        order = jnp.arange(count, dtype=jnp.int32)
        rank = jnp.sum((same & (order[None, :] < order[:, None])).astype(jnp.int32), axis=1)
        cap = -(-(count * 11) // (waves * 8 * 16)) * 16
        fits = jnp.max(rank) < cap
        args = (waves, wave, owner, rank, local_rows, waveforms)
        return lax.cond(
            fits,
            lambda: wave_rows(cap, 0, *args),
            lambda: wave_rows(count, 1, *args),
        )
    picked = jnp.take(waveforms, local_rows, axis=0) * (owner == wave).astype(jnp.float32)[:, None]
    return lax.psum(picked, "wave")


def body(waves, freqs, waveforms, pivots, nodes):
    rows_here, cols_here = waveforms.shape
    steps, size = pivots.shape
    count = steps * size
    col_start = lax.axis_index("freq") * cols_here
    pivot_rows = gather_pivots(waveforms, pivots.reshape(-1), waves)
    columns = col_start + jnp.arange(cols_here, dtype=jnp.int32)
    node_count = jnp.sum((nodes[:, None] == columns[None, :]).astype(jnp.float32), axis=0)
    weighted = pivot_rows * node_count[None, :]
    left = jnp.concatenate([pivot_rows, waveforms], axis=0)
    right = jnp.concatenate([pivot_rows, weighted], axis=0)
    part = jnp.dot(left, right.T, precision=HIGH)
    if freqs == 8:
        total = freq_sum(part, freqs, 2)
    else:
        total = lax.psum(part, "freq")
    mixed = factor(total, steps, size)
    basis_rows = jnp.dot(mixed[:count], pivot_rows, precision=HIGH)
    residual = waveforms - jnp.dot(mixed[count : count + rows_here], pivot_rows, precision=HIGH)
    fitted = jnp.dot(mixed[count + rows_here :], pivot_rows, precision=HIGH)
    return (residual, basis_rows, fitted)


def solution(mesh):
    in_specs = (P("wave", "freq"), P(), P())
    out_specs = (P("wave", "freq"), P(None, "freq"), P("wave", "freq"))
    run = functools.partial(body, mesh.shape["wave"], mesh.shape["freq"])
    return jax.shard_map(run, mesh=mesh, in_specs=in_specs, out_specs=out_specs, check_vma=False)
```

```python
import functools

import jax
import jax.numpy as jnp
from jax import lax
from jax.experimental import pallas as pl
from jax.experimental.pallas import tpu as pltpu
from jax.sharding import PartitionSpec as P

HIGH = lax.Precision.HIGH
FULL = lax.Precision.HIGHEST
MESH = pl.DeviceIdType.MESH
VMEM = pl.BlockSpec(memory_space=pltpu.VMEM)
SMEM = pl.BlockSpec(memory_space=pltpu.SMEM)


def dot(a, b):
    return lax.dot_general(
        a, b, (((1,), (0,)), ((), ())), precision=FULL, preferred_element_type=jnp.float32
    )


def dot_t(a, b):
    return lax.dot_general(
        a, b, (((1,), (1,)), ((), ())), precision=FULL, preferred_element_type=jnp.float32
    )


def factorize(blk, count, total_ref, out_ref, work):
    blocks = count // blk
    subs = lax.broadcasted_iota(jnp.int32, (blk, 2 * blk), 0)
    lanes = lax.broadcasted_iota(jnp.int32, (blk, 2 * blk), 1)
    inner = lax.rem(lanes, blk)
    base = lanes - inner

    cols = [
        [total_ref[c * blk : count, m * count + c * blk : m * count + (c + 1) * blk] for c in range(blocks)]
        for m in range(2)
    ]
    acc = [jnp.zeros((count, count), jnp.float32) for _ in range(2)]
    parts = [[], []]

    def eliminate(j, carry):
        now = work[...]
        row = work[pl.ds(j, 1), :]
        col = jnp.take_along_axis(now, base + j, axis=1)
        pivot = jnp.take_along_axis(jnp.broadcast_to(row, (8, 2 * blk)), base[:8] + j, axis=1)[:1]
        at = inner == j
        row = jnp.where(at[:1], 1.0, row) / pivot
        below = subs > j
        work[...] = jnp.where(at & below, 0.0, now) - jnp.where(below, col, 0.0) * row
        return carry

    for b in range(blocks):
        work[...] = jnp.concatenate([cols[0][b][:blk], cols[1][b][:blk]], axis=1)
        lax.fori_loop(0, blk, eliminate, 0, unroll=4)
        done = work[...]
        for m in range(2):
            mine = done[:, m * blk : (m + 1) * blk]
            sub = lax.broadcasted_iota(jnp.int32, (blk, blk), 0)
            lane = lax.broadcasted_iota(jnp.int32, (blk, blk), 1)
            diag = jnp.sum(jnp.where(sub == lane, mine, 0.0), axis=1, keepdims=True)
            unit = jnp.where(sub > lane, mine, jnp.where(sub == lane, 1.0, 0.0))
            small = unit / jnp.sqrt(diag)
            pads = [jnp.zeros((blk, b * blk), jnp.float32)] if b > 0 else []
            pads.append(small)
            if b + 1 < blocks:
                pads.append(jnp.zeros((blk, count - (b + 1) * blk), jnp.float32))
            wide = jnp.concatenate(pads, axis=1)
            if b > 0:
                wide = wide - dot(small, acc[m][:blk])
            parts[m].append(wide)
            if b + 1 < blocks:
                panel = dot_t(cols[m][b][blk:], small)
                for c in range(b + 1, blocks):
                    low = (c - b - 1) * blk
                    cols[m][c] = cols[m][c] - dot_t(panel[low:], panel[low : low + blk])
                acc[m] = acc[m][blk:] + dot(panel, wide)
    return [jnp.concatenate(p, axis=0) for p in parts]


def factor_kernel(steps, size, total_ref, out_ref, work):
    count = steps * size
    full = factorize(work.shape[0], count, total_ref, out_ref, work)
    out_ref[:count, :] = full[0]
    rows = total_ref.shape[0] - count
    out_ref[count : count + rows, :] = dot(dot_t(total_ref[count:, :count], full[0]), full[0])
    out_ref[count + rows :, :] = dot(dot_t(total_ref[count:, count:], full[1]), full[1])


def factor(total, steps, size):
    count = steps * size
    rows = total.shape[0] - count
    return pl.pallas_call(
        functools.partial(factor_kernel, steps, size),
        out_shape=jax.ShapeDtypeStruct((count + 2 * rows, count), jnp.float32),
        in_specs=[VMEM],
        out_specs=VMEM,
        scratch_shapes=[pltpu.VMEM((size // 2, size), jnp.float32)],
    )(total)


def freq_kernel(chips, part_ref, out_ref, half, near, far, send, recv):
    wave, freq = lax.axis_index("wave"), lax.axis_index("freq")
    core, chip = lax.rem(freq, 2), lax.div(freq, 2)
    rows = part_ref.shape[0]
    mid, piece = rows // 2, rows // 2 // chips
    mate = (wave, chip * 2 + 1 - core)
    others = [(wave, lax.rem(chip + d, chips) * 2 + core) for d in range(1, chips)]
    barrier = pltpu.get_barrier_semaphore()
    for peer in [mate] + others:
        pl.semaphore_signal(barrier, inc=1, device_id=peer, device_id_type=MESH)
    pl.semaphore_wait(barrier, chips)

    def copy(slot, src, dst, peer):
        return pltpu.make_async_remote_copy(
            src_ref=src, dst_ref=dst, send_sem=send.at[slot], recv_sem=recv.at[slot],
            device_id=peer, device_id_type=MESH,
        )

    def span(owner_core, owner_chip):
        return pl.ds(pl.multiple_of(owner_core * mid + owner_chip * piece, 8), piece)

    first = copy(0, part_ref.at[pl.ds(pl.multiple_of((1 - core) * mid, 8), mid)], near, mate)
    first.start()
    first.wait()
    half[...] = part_ref[pl.ds(pl.multiple_of(core * mid, 8), mid), :] + near[...]
    scatter = []
    for d in range(1, chips):
        to = lax.rem(chip + d, chips)
        scatter.append(
            copy(d, half.at[pl.ds(pl.multiple_of(to * piece, 8), piece)], far.at[d - 1], others[d - 1])
        )
        scatter[-1].start()
    for c in scatter:
        c.wait()
    total = half[pl.ds(pl.multiple_of(chip * piece, 8), piece), :]
    for d in range(1, chips):
        total = total + far[d - 1]
    out_ref[span(core, chip), :] = total
    own = out_ref.at[span(core, chip)]
    gather = [copy(chips + d - 1, own, own, others[d - 1]) for d in range(1, chips)]
    for c in gather:
        c.start()
    relay = [copy(2 * chips - 1, own, own, mate)]
    relay[0].start()
    for d in range(1, chips):
        gather[d - 1].wait_recv()
        came = out_ref.at[span(core, lax.rem(chip - d + chips, chips))]
        relay.append(copy(2 * chips - 1 + d, came, came, mate))
        relay[-1].start()
    for c in gather:
        c.wait_send()
    for c in relay:
        c.wait()


def freq_sum(part, freq, ident):
    chips = freq // 2
    rows, cols = part.shape
    slots = 3 * chips - 1
    return pl.pallas_call(
        functools.partial(freq_kernel, chips),
        out_shape=jax.ShapeDtypeStruct(part.shape, part.dtype),
        in_specs=[VMEM],
        out_specs=VMEM,
        scratch_shapes=[
            pltpu.VMEM((rows // 2, cols), jnp.float32),
            pltpu.VMEM((rows // 2, cols), jnp.float32),
            pltpu.VMEM((chips - 1, rows // 2 // chips, cols), jnp.float32),
            pltpu.SemaphoreType.DMA((slots,)),
            pltpu.SemaphoreType.DMA((slots,)),
        ],
        compiler_params=pltpu.CompilerParams(collective_id=ident, has_side_effects=True),
    )(part)


def wave_kernel(take_ref, slot_ref, rows_ref, out_ref, packed, gathered, send, recv, here):
    wave, freq = lax.axis_index("wave"), lax.axis_index("freq")
    y, x = lax.div(wave, 2), lax.rem(wave, 2)
    w_x, w_y = y * 2 + 1 - x, (1 - y) * 2 + x
    cap = packed.shape[0]
    mid = cap // 2
    barrier = pltpu.get_barrier_semaphore()
    for w in (w_x, w_y):
        pl.semaphore_signal(barrier, inc=1, device_id=(w, freq), device_id_type=MESH)

    def pack(k, carry):
        packed[pl.ds(k, 1), :] = rows_ref[pl.ds(take_ref[k], 1), :]
        return carry

    lax.fori_loop(0, cap, pack, 0, unroll=8)
    pl.semaphore_wait(barrier, 2)

    def place(owner, part):
        return gathered.at[pl.ds(pl.multiple_of(owner * cap + part * mid, 8), mid)]

    def copy(slot, src, dst, w):
        return pltpu.make_async_remote_copy(
            src_ref=src, dst_ref=dst, send_sem=send.at[slot], recv_sem=recv.at[slot],
            device_id=(w, freq), device_id_type=MESH,
        )

    def own(part):
        return packed.at[pl.ds(part * mid, mid)]

    x0, x1 = copy(0, own(0), place(wave, 0), w_x), copy(1, own(1), place(wave, 1), w_x)
    y1, y0 = copy(2, own(1), place(wave, 1), w_y), copy(3, own(0), place(wave, 0), w_y)
    for c in (x0, y1, x1, y0):
        c.start()
    stay = pltpu.make_async_copy(packed, gathered.at[pl.ds(pl.multiple_of(wave * cap, 8), cap)], here)
    stay.start()
    x0.wait_recv()
    fy = copy(4, place(w_x, 0), place(w_x, 0), w_y)
    fy.start()
    y1.wait_recv()
    fx = copy(5, place(w_y, 1), place(w_y, 1), w_x)
    fx.start()
    x1.wait_recv()
    y0.wait_recv()
    stay.wait()
    fy.wait_recv()
    fx.wait_recv()
    for c in (x0, x1, y0, y1, fx, fy):
        c.wait_send()

    def unpack(k, carry):
        out_ref[pl.ds(k, 1), :] = gathered[pl.ds(slot_ref[k], 1), :]
        return carry

    lax.fori_loop(0, out_ref.shape[0], unpack, 0, unroll=8)


def wave_rows(cap, ident, waves, wave, owner, rank, local_rows, waveforms):
    count = owner.shape[0]
    cols = waveforms.shape[1]
    order = jnp.arange(cap, dtype=jnp.int32)
    mine = (owner == wave)[None, :] & (rank[None, :] == order[:, None])
    take = jnp.sum(jnp.where(mine, local_rows[None, :], 0), axis=1)
    slot = owner * cap + rank
    return pl.pallas_call(
        wave_kernel,
        out_shape=jax.ShapeDtypeStruct((count, cols), jnp.float32),
        in_specs=[SMEM, SMEM, VMEM],
        out_specs=VMEM,
        scratch_shapes=[
            pltpu.VMEM((cap, cols), jnp.float32),
            pltpu.VMEM((waves * cap, cols), jnp.float32),
            pltpu.SemaphoreType.DMA((6,)),
            pltpu.SemaphoreType.DMA((6,)),
            pltpu.SemaphoreType.DMA,
        ],
        compiler_params=pltpu.CompilerParams(collective_id=ident, has_side_effects=True),
    )(take, slot, waveforms)


def gather_pivots(waveforms, picks, waves):
    rows_here = waveforms.shape[0]
    count = picks.shape[0]
    wave = lax.axis_index("wave")
    owner = lax.div(picks, rows_here)
    local_rows = lax.rem(picks, rows_here)
    if waves == 4:
        same = owner[:, None] == owner[None, :]
        order = jnp.arange(count, dtype=jnp.int32)
        rank = jnp.sum((same & (order[None, :] < order[:, None])).astype(jnp.int32), axis=1)
        cap = -(-(count * 11) // (waves * 8 * 16)) * 16
        fits = jnp.max(rank) < cap
        args = (waves, wave, owner, rank, local_rows, waveforms)
        return lax.cond(
            fits,
            lambda: wave_rows(cap, 0, *args),
            lambda: wave_rows(count, 1, *args),
        )
    picked = jnp.take(waveforms, local_rows, axis=0) * (owner == wave).astype(jnp.float32)[:, None]
    return lax.psum(picked, "wave")


def body(waves, freqs, waveforms, pivots, nodes):
    rows_here, cols_here = waveforms.shape
    steps, size = pivots.shape
    count = steps * size
    col_start = lax.axis_index("freq") * cols_here
    pivot_rows = gather_pivots(waveforms, pivots.reshape(-1), waves)
    columns = col_start + jnp.arange(cols_here, dtype=jnp.int32)
    node_count = jnp.sum((nodes[:, None] == columns[None, :]).astype(jnp.float32), axis=0)
    weighted = pivot_rows * node_count[None, :]
    left = jnp.concatenate([pivot_rows, waveforms], axis=0)
    right = jnp.concatenate([pivot_rows, weighted], axis=0)
    part = jnp.dot(left, right.T, precision=HIGH)
    if freqs == 8:
        total = freq_sum(part, freqs, 2)
    else:
        total = lax.psum(part, "freq")
    mixed = factor(total, steps, size)
    basis_rows = jnp.dot(mixed[:count], pivot_rows, precision=HIGH)
    residual = waveforms - jnp.dot(mixed[count : count + rows_here], pivot_rows, precision=HIGH)
    fitted = jnp.dot(mixed[count + rows_here :], pivot_rows, precision=HIGH)
    return (residual, basis_rows, fitted)


def solution(mesh):
    in_specs = (P("wave", "freq"), P(), P())
    out_specs = (P("wave", "freq"), P(None, "freq"), P("wave", "freq"))
    run = functools.partial(body, mesh.shape["wave"], mesh.shape["freq"])
    return jax.shard_map(run, mesh=mesh, in_specs=in_specs, out_specs=out_specs, check_vma=False)
```

```python
import functools

import jax
import jax.numpy as jnp
from jax import lax
from jax.experimental import pallas as pl
from jax.experimental.pallas import tpu as pltpu
from jax.sharding import PartitionSpec as P

HIGH = lax.Precision.HIGH
FULL = lax.Precision.HIGHEST
MESH = pl.DeviceIdType.MESH
VMEM = pl.BlockSpec(memory_space=pltpu.VMEM)
SMEM = pl.BlockSpec(memory_space=pltpu.SMEM)


def dot(a, b):
    return lax.dot_general(
        a, b, (((1,), (0,)), ((), ())), precision=FULL, preferred_element_type=jnp.float32
    )


def dot_t(a, b):
    return lax.dot_general(
        a, b, (((1,), (1,)), ((), ())), precision=FULL, preferred_element_type=jnp.float32
    )


def factorize(blk, count, fetch, work, between):
    blocks = count // blk
    subs = lax.broadcasted_iota(jnp.int32, (blk, 2 * blk), 0)
    lanes = lax.broadcasted_iota(jnp.int32, (blk, 2 * blk), 1)
    inner = lax.rem(lanes, blk)
    base = lanes - inner

    cols = [
        [fetch(m, c) for c in range(blocks)] for m in range(2)
    ]
    acc = [jnp.zeros((count, count), jnp.float32) for _ in range(2)]
    parts = [[], []]

    def eliminate(j, carry):
        now = work[...]
        row = work[pl.ds(j, 1), :]
        col = jnp.take_along_axis(now, base + j, axis=1)
        pivot = jnp.take_along_axis(jnp.broadcast_to(row, (8, 2 * blk)), base[:8] + j, axis=1)[:1]
        at = inner == j
        row = jnp.where(at[:1], 1.0, row) / pivot
        below = subs > j
        work[...] = jnp.where(at & below, 0.0, now) - jnp.where(below, col, 0.0) * row
        return carry

    for b in range(blocks):
        work[...] = jnp.concatenate([cols[0][b][:blk], cols[1][b][:blk]], axis=1)
        lax.fori_loop(0, blk, eliminate, 0, unroll=4)
        done = work[...]
        for m in range(2):
            mine = done[:, m * blk : (m + 1) * blk]
            sub = lax.broadcasted_iota(jnp.int32, (blk, blk), 0)
            lane = lax.broadcasted_iota(jnp.int32, (blk, blk), 1)
            diag = jnp.sum(jnp.where(sub == lane, mine, 0.0), axis=1, keepdims=True)
            unit = jnp.where(sub > lane, mine, jnp.where(sub == lane, 1.0, 0.0))
            small = unit / jnp.sqrt(diag)
            pads = [jnp.zeros((blk, b * blk), jnp.float32)] if b > 0 else []
            pads.append(small)
            if b + 1 < blocks:
                pads.append(jnp.zeros((blk, count - (b + 1) * blk), jnp.float32))
            wide = jnp.concatenate(pads, axis=1)
            if b > 0:
                wide = wide - dot(small, acc[m][:blk])
            parts[m].append(wide)
            if b + 1 < blocks:
                panel = dot_t(cols[m][b][blk:], small)
                for c in range(b + 1, blocks):
                    low = (c - b - 1) * blk
                    cols[m][c] = cols[m][c] - dot_t(panel[low:], panel[low : low + blk])
                acc[m] = acc[m][blk:] + dot(panel, wide)
        between(b)
    return [jnp.concatenate(p, axis=0) for p in parts]


def solve(full, cross, rows, count, out_ref):
    out_ref[:count, :] = full[0]
    out_ref[count : count + rows, :] = dot(dot_t(cross[:, :count], full[0]), full[0])
    out_ref[count + rows :, :] = dot(dot_t(cross[:, count:], full[1]), full[1])


def factor_kernel(count, total_ref, out_ref, work):
    blk = work.shape[0]

    def fetch(m, c):
        return total_ref[c * blk : count, m * count + c * blk : m * count + (c + 1) * blk]

    full = factorize(blk, count, fetch, work, lambda b: None)
    solve(full, total_ref[count:, :], total_ref.shape[0] - count, count, out_ref)


def factor(total, count):
    rows = total.shape[0] - count
    return pl.pallas_call(
        functools.partial(factor_kernel, count),
        out_shape=jax.ShapeDtypeStruct((count + 2 * rows, count), jnp.float32),
        in_specs=[VMEM],
        out_specs=VMEM,
        scratch_shapes=[pltpu.VMEM((64, 128), jnp.float32)],
    )(total)


def sum_factor_kernel(
    chips, count, part_ref, out_ref, near_g, half_g, far_g, gram, near_x, half_x, far_x, cross, work, send, recv
):
    wave, freq = lax.axis_index("wave"), lax.axis_index("freq")
    core, chip = lax.rem(freq, 2), lax.div(freq, 2)
    size = count // 2
    tall = 3 * size
    step_g = tall // chips
    rows = part_ref.shape[0] - count
    mid = rows // 2
    step_x = mid // chips
    mate = (wave, chip * 2 + 1 - core)
    others = [(wave, lax.rem(chip + d, chips) * 2 + core) for d in range(1, chips)]
    barrier = pltpu.get_barrier_semaphore()
    for peer in [mate] + others:
        pl.semaphore_signal(barrier, inc=1, device_id=peer, device_id_type=MESH)
    pl.semaphore_wait(barrier, chips)
    used = [0]

    def copy(src, dst, peer):
        slot = used[0]
        used[0] += 1
        return pltpu.make_async_remote_copy(
            src_ref=src, dst_ref=dst, send_sem=send.at[slot], recv_sem=recv.at[slot],
            device_id=peer, device_id_type=MESH,
        )

    def at(start, length):
        return pl.ds(pl.multiple_of(start, 8), length)

    def block(i, owner):
        row, col = ((0, 0), (1, 0), (1, 1))[i]
        return pl.ds(row * size, size), pl.ds(pl.multiple_of(owner * count + col * size, 128), size)

    swaps = [copy(part_ref.at[block(i, 1 - core)], near_g.at[pl.ds(i * size, size)], mate) for i in range(3)]
    swap_x = copy(part_ref.at[at(count + (1 - core) * mid, mid)], near_x, mate)
    for c in swaps:
        c.start()
    swap_x.start()

    def all_to_all(half, far, step):
        return [
            copy(half.at[at(lax.rem(chip + d, chips) * step, step)], far.at[d - 1], others[d - 1])
            for d in range(1, chips)
        ]

    def gathered(whole, tall, step):
        own = whole.at[at(core * tall + chip * step, step)]
        return [copy(own, own, others[d - 1]) for d in range(1, chips)], copy(own, own, mate)

    def relays(whole, tall, step):
        out = []
        for d in range(1, chips):
            came = whole.at[at(core * tall + lax.rem(chip - d + chips, chips) * step, step)]
            out.append(copy(came, came, mate))
        return out

    def reduce(half, far, step):
        total = half[at(chip * step, step), :]
        for d in range(1, chips):
            total = total + far[d - 1]
        return total

    for i in range(3):
        swaps[i].wait_recv()
        here = pl.ds(i * size, size)
        half_g[here, :] = part_ref[block(i, core)] + near_g[here, :]
    scatter_g = all_to_all(half_g, far_g, step_g)
    for c in scatter_g:
        c.start()
    swap_x.wait_recv()
    half_x[...] = part_ref[at(count + core * mid, mid), :] + near_x[...]
    for c in scatter_g:
        c.wait_recv()
    gram[at(core * tall + chip * step_g, step_g), :] = reduce(half_g, far_g, step_g)
    sends_g, mate_g = gathered(gram, tall, step_g)
    for c in sends_g:
        c.start()
    mate_g.start()
    scatter_x = all_to_all(half_x, far_x, step_x)
    for c in scatter_x:
        c.start()
    relay_g = relays(gram, tall, step_g)
    for d in range(chips - 1):
        sends_g[d].wait_recv()
        relay_g[d].start()
    mate_g.wait_recv()
    for c in relay_g:
        c.wait_recv()
    sends_x, mate_x = gathered(cross, mid, step_x)
    relay_x = relays(cross, mid, step_x)
    blk = work.shape[0]

    def fetch(m, c):
        top = m * tall
        low = c * blk
        if low < size:
            return gram[top + low : top + 2 * size, low : low + blk]
        return gram[top + size + low : top + tall, low - size : low - size + blk]

    def between(b):
        if b == 1:
            for c in scatter_x:
                c.wait_recv()
            cross[at(core * mid + chip * step_x, step_x), :] = reduce(half_x, far_x, step_x)
            for c in sends_x:
                c.start()
            mate_x.start()
        if b == 3:
            for d in range(chips - 1):
                sends_x[d].wait_recv()
                relay_x[d].start()

    full = factorize(blk, count, fetch, work, between)
    mate_x.wait_recv()
    for c in relay_x:
        c.wait_recv()
    solve(full, cross[...], rows, count, out_ref)
    for c in swaps + [swap_x, mate_g, mate_x] + scatter_g + scatter_x + sends_g + sends_x + relay_g + relay_x:
        c.wait_send()


def sum_factor(part, count, freq, ident):
    chips = freq // 2
    rows = part.shape[0] - count
    size = count // 2
    tall = 3 * size
    cols = part.shape[1]
    slots = 4 + 6 * (chips - 1) + 2

    def buffer(*shape):
        return pltpu.VMEM(shape, jnp.float32)

    return pl.pallas_call(
        functools.partial(sum_factor_kernel, chips, count),
        out_shape=jax.ShapeDtypeStruct((count + 2 * rows, count), jnp.float32),
        in_specs=[VMEM],
        out_specs=VMEM,
        scratch_shapes=[
            buffer(tall, size),
            buffer(tall, size),
            buffer(chips - 1, tall // chips, size),
            buffer(2 * tall, size),
            buffer(rows // 2, cols),
            buffer(rows // 2, cols),
            buffer(chips - 1, rows // 2 // chips, cols),
            buffer(rows, cols),
            buffer(64, 128),
            pltpu.SemaphoreType.DMA((slots,)),
            pltpu.SemaphoreType.DMA((slots,)),
        ],
        compiler_params=pltpu.CompilerParams(collective_id=ident, has_side_effects=True),
    )(part)


def wave_kernel(take_ref, slot_ref, rows_ref, out_ref, packed, gathered, send, recv, here):
    wave, freq = lax.axis_index("wave"), lax.axis_index("freq")
    y, x = lax.div(wave, 2), lax.rem(wave, 2)
    w_x, w_y = y * 2 + 1 - x, (1 - y) * 2 + x
    cap = packed.shape[0]
    mid = cap // 2
    barrier = pltpu.get_barrier_semaphore()
    for w in (w_x, w_y):
        pl.semaphore_signal(barrier, inc=1, device_id=(w, freq), device_id_type=MESH)

    def pack(k, carry):
        packed[pl.ds(k, 1), :] = rows_ref[pl.ds(take_ref[k], 1), :]
        return carry

    lax.fori_loop(0, mid, pack, 0, unroll=8)
    pl.semaphore_wait(barrier, 2)

    def place(owner, part):
        return gathered.at[pl.ds(pl.multiple_of(owner * cap + part * mid, 8), mid)]

    def copy(slot, src, dst, w):
        return pltpu.make_async_remote_copy(
            src_ref=src, dst_ref=dst, send_sem=send.at[slot], recv_sem=recv.at[slot],
            device_id=(w, freq), device_id_type=MESH,
        )

    def own(part):
        return packed.at[pl.ds(part * mid, mid)]

    x0, x1 = copy(0, own(0), place(wave, 0), w_x), copy(1, own(1), place(wave, 1), w_x)
    y1, y0 = copy(2, own(1), place(wave, 1), w_y), copy(3, own(0), place(wave, 0), w_y)
    x0.start()
    lax.fori_loop(mid, cap, pack, 0, unroll=8)
    for c in (y1, x1, y0):
        c.start()
    stay = pltpu.make_async_copy(packed, gathered.at[pl.ds(pl.multiple_of(wave * cap, 8), cap)], here)
    stay.start()
    x0.wait_recv()
    fy = copy(4, place(w_x, 0), place(w_x, 0), w_y)
    fy.start()
    y1.wait_recv()
    fx = copy(5, place(w_y, 1), place(w_y, 1), w_x)
    fx.start()
    x1.wait_recv()
    y0.wait_recv()
    stay.wait()
    fy.wait_recv()
    fx.wait_recv()
    for c in (x0, x1, y0, y1, fx, fy):
        c.wait_send()

    def unpack(k, carry):
        out_ref[pl.ds(k, 1), :] = gathered[pl.ds(slot_ref[k], 1), :]
        return carry

    lax.fori_loop(0, out_ref.shape[0], unpack, 0, unroll=8)


def wave_rows(cap, ident, waves, wave, owner, rank, local_rows, waveforms):
    count = owner.shape[0]
    cols = waveforms.shape[1]
    order = jnp.arange(cap, dtype=jnp.int32)
    mine = (owner == wave)[None, :] & (rank[None, :] == order[:, None])
    take = jnp.sum(jnp.where(mine, local_rows[None, :], 0), axis=1)
    slot = owner * cap + rank
    return pl.pallas_call(
        wave_kernel,
        out_shape=jax.ShapeDtypeStruct((count, cols), jnp.float32),
        in_specs=[SMEM, SMEM, VMEM],
        out_specs=VMEM,
        scratch_shapes=[
            pltpu.VMEM((cap, cols), jnp.float32),
            pltpu.VMEM((waves * cap, cols), jnp.float32),
            pltpu.SemaphoreType.DMA((6,)),
            pltpu.SemaphoreType.DMA((6,)),
            pltpu.SemaphoreType.DMA,
        ],
        compiler_params=pltpu.CompilerParams(collective_id=ident, has_side_effects=True),
    )(take, slot, waveforms)


def gather_pivots(waveforms, picks, waves):
    rows_here = waveforms.shape[0]
    count = picks.shape[0]
    wave = lax.axis_index("wave")
    owner = lax.div(picks, rows_here)
    local_rows = lax.rem(picks, rows_here)
    if waves == 4:
        same = owner[:, None] == owner[None, :]
        order = jnp.arange(count, dtype=jnp.int32)
        rank = jnp.sum((same & (order[None, :] < order[:, None])).astype(jnp.int32), axis=1)
        caps = [-(-count * 5 // (waves * 64)) * 16, -(-count * 3 // (waves * 32)) * 16, count]
        most = jnp.max(rank) + 1
        args = (waves, wave, owner, rank, local_rows, waveforms)
        tier = jnp.sum((most > jnp.array(caps[:-1])).astype(jnp.int32))
        return lax.switch(tier, [functools.partial(wave_rows, cap, i, *args) for i, cap in enumerate(caps)])
    picked = jnp.take(waveforms, local_rows, axis=0) * (owner == wave).astype(jnp.float32)[:, None]
    return lax.psum(picked, "wave")


def body(waves, freqs, waveforms, pivots, nodes):
    rows_here, cols_here = waveforms.shape
    steps, size = pivots.shape
    count = steps * size
    col_start = lax.axis_index("freq") * cols_here
    pivot_rows = gather_pivots(waveforms, pivots.reshape(-1), waves)
    columns = col_start + jnp.arange(cols_here, dtype=jnp.int32)
    node_count = jnp.sum((nodes[:, None] == columns[None, :]).astype(jnp.float32), axis=0)
    weighted = pivot_rows * node_count[None, :]
    left = jnp.concatenate([pivot_rows, waveforms], axis=0)
    right = jnp.concatenate([pivot_rows, weighted], axis=0)
    part = jnp.dot(left, right.T, precision=HIGH)
    if freqs == 8 and count == 256:
        mixed = sum_factor(part, count, freqs, 3)
    else:
        mixed = factor(lax.psum(part, "freq"), count)
    basis_rows = jnp.dot(mixed[:count], pivot_rows, precision=HIGH)
    residual = waveforms - jnp.dot(mixed[count : count + rows_here], pivot_rows, precision=HIGH)
    fitted = jnp.dot(mixed[count + rows_here :], pivot_rows, precision=HIGH)
    return (residual, basis_rows, fitted)


def solution(mesh):
    in_specs = (P("wave", "freq"), P(), P())
    out_specs = (P("wave", "freq"), P(None, "freq"), P("wave", "freq"))
    run = functools.partial(body, mesh.shape["wave"], mesh.shape["freq"])
    return jax.shard_map(run, mesh=mesh, in_specs=in_specs, out_specs=out_specs, check_vma=False)
```
